32 devices in a mesh: row: 16 (over z, y, x), col: 2 (over core).
Axes of the slice: x: 2, y: 2, z: 4, core: 2. Of those that a mesh axis runs over, the one named last changes fastest.
Arguments:
- eri_cols: float32 [8192, 512], P('row'), as said below
- old_factor: float32 [8192, 1024], P('row', 'col')
- residual_diag: float32 [8192], P('row'), as said below
- pivots: int32 [4, 128], replicated, may hold values from 0 to 8191, as said below
- row_ids: int32 [8192], P('row'), may hold values from 0 to 8191, as said below
Outputs:
- panels: float32 [8192, 512], P('row')
- new_diag: float32 [8192], P('row')
The draws below stay inside these ranges and needn't reach their ends.
Inputs may be any that keep to these rules, and one draw needn't show every extreme that they name: `pivots`: 512 distinct pair indices, each held by some stored row. `row_ids`: every pair index held by exactly one stored row. `eri_cols`: the pair matrix minus the earlier factor's product is symmetric positive definite on the pivots, with smallest eigenvalue 0.25 or more. `residual_diag`: the diagonal of the same residual matrix whose pivot columns eri_cols holds.
All inputs are finite; a program needn't handle non-finite values.
Results may differ from the reference program's by a relative error of at most 0.0003.
Values sent between devices are 32-bit elements; how exact they have to be, the bound alone decides.
A program may use at most 64 MiB of HBM per device.

```python
import math
import jax
import jax.numpy as jnp
from jax import lax

NB = 128
STEPS = 4
KOLD = 1024
PAIRS = 8192
PIVOTS = 512
RANK_W = 640


def integer_parts(key):
    row_ids = jax.random.permutation(jax.random.fold_in(key, 11), PAIRS).astype(jnp.int32)
    places = jax.random.permutation(jax.random.fold_in(key, 12), PAIRS)[:PIVOTS].astype(jnp.int32)
    pivots = row_ids[places].reshape(STEPS, NB)
    return (row_ids, places, pivots)


def float_parts(key):
    row_ids, places, pivots = integer_parts(key)
    old = jax.random.normal(jax.random.fold_in(key, 22), (PAIRS, KOLD)) / math.sqrt(KOLD)
    remain = jax.random.normal(jax.random.fold_in(key, 25), (PAIRS, RANK_W)) / math.sqrt(RANK_W)
    exact = lax.Precision.HIGHEST
    ident = (jnp.arange(PAIRS, dtype=jnp.int32)[:, None] == places[None, :]).astype(jnp.float32)
    eri = jnp.dot(old, old[places].T, precision=exact) + jnp.dot(remain, remain[places].T, precision=exact) + 0.25 * ident
    diagonal = jnp.sum(remain * remain, axis=1) + 0.25
    return (eri.astype(jnp.float32), old.astype(jnp.float32), diagonal.astype(jnp.float32))


def draw_eri_cols(key, part):
    return float_parts(key)[0]


def draw_old_factor(key, part):
    return float_parts(key)[1]


def draw_residual_diag(key, part):
    return float_parts(key)[2]


def draw_pivots(key, part):
    return integer_parts(key)[2]


def draw_row_ids(key, part):
    return integer_parts(key)[0]


def setup_inputs(seed: int = 0) -> dict:
    keys = jax.random.split(jax.random.key(seed), 6)
    eri_cols = draw_eri_cols(jax.random.fold_in(keys[5], 71), 0)
    old_factor = draw_old_factor(jax.random.fold_in(keys[5], 71), 0)
    residual_diag = draw_residual_diag(jax.random.fold_in(keys[5], 71), 0)
    pivots = draw_pivots(jax.random.fold_in(keys[5], 71), 0)
    row_ids = draw_row_ids(jax.random.fold_in(keys[5], 71), 0)
    return dict(eri_cols=eri_cols, old_factor=old_factor, residual_diag=residual_diag, pivots=pivots, row_ids=row_ids)


def reference(eri_cols, old_factor, residual_diag, pivots, row_ids):
    exact = lax.Precision.HIGHEST
    pairs = row_ids.shape[0]
    inverse = jnp.zeros((pairs,), jnp.int32).at[row_ids].set(jnp.arange(pairs, dtype=jnp.int32))
    places = inverse[pivots.reshape(-1).astype(jnp.int32)].astype(jnp.int32)
    old_rows = old_factor[places]
    reduced = eri_cols - jnp.dot(old_factor.astype(jnp.float32), old_rows.T.astype(jnp.float32), precision=exact, preferred_element_type=jnp.float32)
    width = pivots.shape[1]
    diagonal = residual_diag
    outputs = []
    for step in range(pivots.shape[0]):
        wanted = places[step * width:(step + 1) * width]
        columns = reduced[:, step * width:(step + 1) * width]
        if step > 0:
            earlier = jnp.concatenate(outputs, axis=1)
            columns = columns - jnp.dot(earlier.astype(jnp.float32), earlier[wanted].T.astype(jnp.float32), precision=exact, preferred_element_type=jnp.float32)
        factor_block = jnp.linalg.cholesky(columns[wanted])
        new_panel = lax.linalg.triangular_solve(factor_block, columns, left_side=False, lower=True, transpose_a=True)
        diagonal = diagonal - jnp.sum(new_panel * new_panel, axis=1)
        outputs.append(new_panel)
    return (jnp.concatenate(outputs, axis=1), diagonal)
```

```python
import functools
import jax
import jax.numpy as jnp
from jax import lax
from jax.experimental import pallas as pl
from jax.experimental.pallas import tpu as pltpu
from jax.sharding import PartitionSpec as P

ROWS_T = (((1,), (1,)), ((), ()))
SUB = 8


def split(x):
    hi = x.astype(jnp.bfloat16)
    return hi, (x - hi.astype(jnp.float32)).astype(jnp.bfloat16)


def dot_t(a, b):
    f = functools.partial(
        lax.dot_general, dimension_numbers=ROWS_T, preferred_element_type=jnp.float32
    )
    return f(a[0], b[0]) + (f(a[0], b[1]) + f(a[1], b[0]))


def inverse_factor(a):
    n = a.shape[0]
    groups = n // SUB
    row = lax.broadcasted_iota(jnp.int32, (SUB, n), 0)
    lane = lax.broadcasted_iota(jnp.int32, (SUB, n), 1)
    A = [a[SUB * i : SUB * i + SUB, :] for i in range(groups)]
    W = [jnp.where(lane == row + SUB * i, 1.0, 0.0) for i in range(groups)]
    out = []
    wide = lambda v: jnp.broadcast_to(v, (SUB, n))
    for g in range(groups):
        j = SUB * g
        C = [[wide(A[i][:, j + k : j + k + 1]) for k in range(SUB)] for i in range(g, groups)]
        D = [[wide(C[0][l][k : k + 1, :]) for l in range(k + 1)] for k in range(SUB)]
        r = [wide(A[g][k : k + 1, :]) for k in range(SUB)]
        w = [wide(W[g][k : k + 1, :]) for k in range(SUB)]
        inv, m = [], [[None] * SUB for _ in range(SUB)]
        done = jnp.zeros((SUB, n), jnp.float32)
        for k in range(SUB):
            root = lax.rsqrt(D[k][k])
            inv.append(root * root)
            done = jnp.where(row == k, w[k] * root, done)
            for i in range(k + 1, SUB):
                m[i][k] = D[i][k] * inv[k]
            for i in range(k + 1, SUB):
                for l in range(k + 1, i + 1):
                    D[i][l] = D[i][l] - m[i][k] * D[l][k]
                r[i] = r[i] - m[i][k] * r[k]
                w[i] = w[i] - m[i][k] * w[k]
        out.append(done)
        if g + 1 == groups:
            break
        s, t = [None] * SUB, [None] * SUB
        for k in reversed(range(SUB)):
            s[k], t[k] = r[k] * inv[k], w[k] * inv[k]
            for i in reversed(range(k + 1, SUB)):
                s[k] = s[k] - m[i][k] * s[i]
                t[k] = t[k] - m[i][k] * t[i]
        for i in range(g + 1, groups):
            c = C[i - g]
            for k in range(SUB):
                A[i] = A[i] - c[k] * s[k]
                W[i] = W[i] - c[k] * t[k]
    return jnp.concatenate(out, axis=0)


def factor_kernel(steps, pivot_ref, rows_ref, diag_ref, panel_ref, new_ref, work):
    piv = pivot_ref.shape[0]
    width = piv // steps
    work[:piv, :] = pivot_ref[...]
    work[piv:, :] = rows_ref[...]
    new_ref[...] = diag_ref[...]
    ones = jnp.ones((SUB, width), jnp.bfloat16)

    def step(s, carry):
        at = pl.ds(pl.multiple_of(s * width, width), width)
        inv = split(inverse_factor(work[at, at]))
        solved = dot_t(split(work[:, at]), inv)
        own = solved[piv:]
        panel_ref[:, at] = own
        hi, lo = split(own * own)
        f = functools.partial(
            lax.dot_general, dimension_numbers=ROWS_T, preferred_element_type=jnp.float32
        )
        new_ref[...] -= (f(ones, hi) + f(ones, lo))[:1]

        @pl.when(s < steps - 1)
        def _():
            both = split(solved)
            work[...] -= dot_t(both, (both[0][:piv], both[1][:piv]))

        return carry

    lax.fori_loop(0, steps, step, 0)


def factor(pivot_rows, reduced, diagonal, steps):
    piv, rows = pivot_rows.shape[0], reduced.shape[0]
    panels, new = pl.pallas_call(
        functools.partial(factor_kernel, steps),
        out_shape=(
            jax.ShapeDtypeStruct((rows, piv), jnp.float32),
            jax.ShapeDtypeStruct((1, rows), jnp.float32),
        ),
        in_specs=[pl.BlockSpec(memory_space=pltpu.VMEM)] * 3,
        out_specs=[pl.BlockSpec(memory_space=pltpu.VMEM)] * 2,
        scratch_shapes=[pltpu.VMEM((piv + rows, piv), jnp.float32)],
        compiler_params=pltpu.CompilerParams(vmem_limit_bytes=40 * 1024 * 1024),
        name="factor",
    )(pivot_rows, reduced, diagonal[None, :])
    return panels, new[0]


def pick_rows(wanted, row_ids, arrays):
    matches = wanted[:, None] == row_ids[None, :]
    slots = jnp.sum(
        jnp.where(matches, lax.broadcasted_iota(jnp.int32, matches.shape, 1), 0), axis=1
    )
    present = jnp.any(matches, axis=1)[:, None]
    return tuple((jnp.where(present, jnp.take(source, slots, axis=0), 0.0) for source in arrays))


def product(left, right):
    return jnp.dot(
        left, right.T, precision=lax.Precision.HIGHEST, preferred_element_type=jnp.float32
    )


def on_device(eri_cols, old_factor, residual_diag, pivots, row_ids):
    every_pivot = pivots.reshape(-1)
    old_rows, eri_rows = pick_rows(every_pivot, row_ids, (old_factor, eri_cols))
    old_rows, eri_rows = lax.psum((old_rows, eri_rows), "row")
    old_cross, old_gram = lax.psum(
        (product(old_factor, old_rows), product(old_rows, old_rows)), "col"
    )
    return factor(
        eri_rows - old_gram, eri_cols - old_cross, residual_diag, pivots.shape[0]
    )


def solution(mesh):
    placed = (P("row", None), P("row", "col"), P("row"), P(), P("row"))
    return jax.shard_map(
        on_device, mesh=mesh, in_specs=placed, out_specs=(P("row", None), P("row")), check_vma=False
    )
```
